256 devices in a mesh: rep: 2 (over z), kv: 128 (over x, y, core).
Axes of the slice: x: 8, y: 8, z: 2, core: 2. Of those that a mesh axis runs over, the one named last changes fastest.
The devices are a block of a 8x8x16 slice.
Arguments:
- queries: bfloat16 [32, 3, 36864], P('rep', None, 'kv'), parts along dimension 0, may hold values from -4 to 4
- cache: bfloat16 [65536, 16, 576], P(('rep', 'kv')), parts along dimension 0, may hold values from -4 to 4
- page_counts: int32 [32], P('rep'), parts along dimension 0, may hold values from 1 to 16384, as said below
- slot_request: int32 [8192], P(('rep', 'kv')), parts along dimension 0, may hold values from 0 to 15, as said below
- slot_start: int32 [8192], P(('rep', 'kv')), parts along dimension 0, may hold values from 0 to 16376, as said below
- slot_live: int32 [8192], P(('rep', 'kv')), parts along dimension 0, may hold values from 1 to 8, as said below
- slot_pages: int32 [8192, 8], P(('rep', 'kv')), parts along dimension 0, may hold values from 0 to 255, as said below
Outputs:
- attended: bfloat16 [32, 3, 32768], P('rep', None, 'kv'), parts along dimension 0
- lse: float32 [32, 3, 64], P('rep'), parts along dimension 0
The draws below stay inside these ranges and needn't reach their ends.
There are 2 independent parts, one for each index of `rep`. The reference program is written for one: setup_inputs(seed, part) draws one part's arguments, and reference() takes and returns one part's arrays. A program takes and returns all parts, laid end to end along the dimension named above; each array names one. Nothing has to cross between parts.
Inputs may be any that keep to these rules, and one draw needn't show every extreme that they name: Request r has 16 * page_counts[r] tokens; the slots that name r cover its pages 0 to page_counts[r] - 1, each exactly once; one request holds 8 * (2048) pages. `slot_request`: every request is named by at least one slot; slot s lives on index s // 32 of kv. Slot s covers pages slot_start[s] to slot_start[s] + slot_live[s] - 1 of its request. Only the first slot_live[s] entries of slot_pages[s] are used. `slot_pages`: page numbers local to the device that holds the slot; all entries of one device's slots are distinct.
All inputs are finite; a program needn't handle non-finite values.
Results may differ from the reference program's by a relative error of at most 0.0043.
Values may be sent and summed in bfloat16 or wider, within the bound.
A program may use at most 128 MiB of HBM per device.

```python
import jax
import jax.numpy as jnp
import numpy as np
from jax import lax

H = 64
LAT = 512
ROPE = 64
PAGE = 16
SPAN = 8
QN = 3
REQS = 16
ITEMS = 32
P_DEV = 256
SLOTS = 4096
PAGES = 32768


def plan_tables(key):
    heavy = SLOTS // 2
    weights = np.array([720720 // ((position + 2) * (position + 2)) for position in range(REQS - 1)], dtype=np.int64)
    spare = SLOTS - heavy - (REQS - 1)
    rest = spare * weights // weights.sum() + 1
    rest[0] += SLOTS - heavy - rest.sum()
    shares = np.concatenate([np.array([heavy], dtype=np.int64), rest])
    bounds = np.cumsum(shares)
    firsts = bounds - shares
    rank_at = np.searchsorted(bounds, np.arange(SLOTS), side='right').astype(np.int32)
    base_key = jax.random.fold_in(key, 1234)
    order_key, request_key, live_key, page_key = jax.random.split(base_key, 4)
    order = jax.random.permutation(order_key, SLOTS)
    request_perm = jax.random.permutation(request_key, REQS).astype(jnp.int32)
    request_at = request_perm[rank_at]
    live_drawn = jax.random.randint(live_key, (SLOTS,), 1, SPAN + 1).astype(jnp.int32)
    live_at = jnp.where(jnp.asarray(rank_at) == 0, SPAN, live_drawn).astype(jnp.int32)
    running = jnp.cumsum(live_at) - live_at
    start_at = running - running[firsts][rank_at]
    page_totals = running[bounds - 1] + live_at[bounds - 1] - running[firsts]
    page_counts = jnp.zeros((REQS,), jnp.int32).at[request_perm].set(page_totals.astype(jnp.int32))
    slot_request = jnp.zeros((SLOTS,), jnp.int32).at[order].set(request_at)
    slot_start = jnp.zeros((SLOTS,), jnp.int32).at[order].set(start_at.astype(jnp.int32))
    slot_live = jnp.zeros((SLOTS,), jnp.int32).at[order].set(live_at)
    device_count = SLOTS // ITEMS
    page_keys = jax.random.split(page_key, device_count)
    local_perm = jax.vmap(lambda one_key: jax.random.permutation(one_key, P_DEV))(page_keys)
    slot_pages = local_perm.reshape(SLOTS, SPAN).astype(jnp.int32)
    return (page_counts, slot_request, slot_start, slot_live, slot_pages)


def draw_queries(key, part):
    array_shape = (REQS, QN, H, LAT + ROPE)
    values = jax.random.truncated_normal(jax.random.fold_in(key, 11), -4.0, 4.0, array_shape, jnp.float32)
    return values.reshape(REQS, QN, H * (LAT + ROPE)).astype(jnp.bfloat16)


def draw_cache(key, part):
    array_shape = (PAGES, PAGE, LAT + ROPE)
    values = jax.random.truncated_normal(jax.random.fold_in(key, 22), -4.0, 4.0, array_shape, jnp.float32)
    return values.astype(jnp.bfloat16)


def draw_page_counts(key, part):
    return plan_tables(key)[0]


def draw_slot_request(key, part):
    return plan_tables(key)[1]


def draw_slot_start(key, part):
    return plan_tables(key)[2]


def draw_slot_live(key, part):
    return plan_tables(key)[3]


def draw_slot_pages(key, part):
    return plan_tables(key)[4]


def setup_inputs(seed: int = 0, part: int = 0) -> dict:
    streams_of = jax.random.split(jax.random.key(seed), 8)
    own_keys = jax.random.split(jax.random.fold_in(streams_of[7], part), 8)
    return {
        "queries": draw_queries(jax.random.fold_in(jax.random.fold_in(streams_of[7], part), 71), part),
        "cache": draw_cache(jax.random.fold_in(jax.random.fold_in(streams_of[7], part), 71), part),
        "page_counts": draw_page_counts(jax.random.fold_in(jax.random.fold_in(streams_of[7], part), 71), part),
        "slot_request": draw_slot_request(jax.random.fold_in(jax.random.fold_in(streams_of[7], part), 71), part),
        "slot_start": draw_slot_start(jax.random.fold_in(jax.random.fold_in(streams_of[7], part), 71), part),
        "slot_live": draw_slot_live(jax.random.fold_in(jax.random.fold_in(streams_of[7], part), 71), part),
        "slot_pages": draw_slot_pages(jax.random.fold_in(jax.random.fold_in(streams_of[7], part), 71), part),
    }


softmax_scale = 192.0 ** -0.5
neg_floor = -1.0e30


def slot_partials(query_heads, key_rows, request, first_page, live_pages, page_counts, page_rows, latent):
    row_count = key_rows.shape[1]
    query_count = query_heads.shape[1]
    chosen = query_heads[request].astype(jnp.float32)
    scores = jnp.einsum("gqhc,gjc->gqhj", chosen, key_rows.astype(jnp.float32)) * softmax_scale
    row_ids = jnp.arange(row_count, dtype=jnp.int32)
    page_of = row_ids // page_rows
    position = (first_page[:, None] + page_of[None, :]) * page_rows + row_ids[None, :] % page_rows
    request_pages = page_counts[request]
    query_ids = jnp.arange(query_count, dtype=jnp.int32)
    limit = request_pages[:, None] * page_rows - (query_count - 1 - query_ids)[None, :]
    visible = (page_of[None, None, :] < live_pages[:, None, None]) & (position[:, None, :] < limit[:, :, None])
    visible = visible[:, :, None, :]
    slot_max = jnp.max(jnp.where(visible, scores, neg_floor), axis=3)
    shifted = jnp.where(visible, scores - slot_max[..., None], neg_floor)
    weights = jnp.exp(shifted)
    slot_sum = jnp.sum(weights, axis=3)
    rounded = weights.astype(jnp.bfloat16)
    slot_out = jnp.einsum("gqhj,gjc->gqhc", rounded.astype(jnp.float32), key_rows[:, :, :latent].astype(jnp.float32))
    return slot_max, slot_sum, slot_out


def fold_slots(carry, request, slot_max, slot_sum, slot_out):
    best, denom, numer = carry
    request_count = best.shape[0]
    member = request[:, None] == jnp.arange(request_count, dtype=jnp.int32)[None, :]
    block_best = jnp.max(jnp.where(member[:, :, None, None], slot_max[:, None], neg_floor), axis=0)
    new_best = jnp.maximum(best, block_best)
    kept = jnp.exp(best - new_best)
    member_float = member.astype(jnp.float32)
    factor = jnp.exp(slot_max - new_best[request])
    denom = denom * kept + jnp.einsum("gr,gqh->rqh", member_float, factor * slot_sum, precision=lax.Precision.HIGHEST)
    numer = numer * kept[..., None] + jnp.einsum("gr,gqhc->rqhc", member_float, factor[..., None] * slot_out, precision=lax.Precision.HIGHEST)
    return new_best, denom, numer


def reference(queries, cache, page_counts, slot_request, slot_start, slot_live, slot_pages):
    request_count, query_count, _flat = queries.shape
    token_width = LAT + ROPE
    query_heads = queries.reshape(request_count, query_count, H, token_width)
    owner_base = (jnp.arange(SLOTS, dtype=jnp.int32) // ITEMS) * P_DEV
    global_pages = (slot_pages + owner_base[:, None]).astype(jnp.int32)
    step_count = SLOTS // ITEMS
    inputs = (slot_request.reshape(step_count, ITEMS), slot_start.reshape(step_count, ITEMS),
              slot_live.reshape(step_count, ITEMS), global_pages.reshape(step_count, ITEMS, SPAN))
    initial = (jnp.full((request_count, query_count, H), neg_floor, jnp.float32),
               jnp.zeros((request_count, query_count, H), jnp.float32),
               jnp.zeros((request_count, query_count, H, LAT), jnp.float32))

    def one_step(carry, pieces):
        request, first_page, live_pages, pages = pieces
        key_rows = cache[pages.reshape(-1)].reshape(ITEMS, SPAN * PAGE, token_width)
        slot_max, slot_sum, slot_out = slot_partials(query_heads, key_rows, request, first_page, live_pages, page_counts, PAGE, LAT)
        dev_best, dev_denom, dev_numer = fold_slots(initial, request, slot_max, slot_sum, slot_out)
        dev_partial = lax.optimization_barrier(dev_numer.astype(jnp.bfloat16)).astype(jnp.float32)
        best, denom, numer = carry
        new_best = jnp.maximum(best, dev_best)
        kept = jnp.exp(best - new_best)
        added = jnp.exp(dev_best - new_best)
        denom = denom * kept + dev_denom * added
        numer = numer * kept[..., None] + dev_partial * added[..., None]
        return (new_best, denom, numer), None

    (best, denom, numer), _unused = lax.scan(one_step, initial, inputs)
    attended = (numer / denom[..., None]).reshape(request_count, query_count, H * LAT).astype(jnp.bfloat16)
    lse = best + jnp.log(denom)
    return attended, lse
```

```python
import functools

import jax
import jax.numpy as jnp
from jax import lax
from jax.experimental import pallas as pl
from jax.experimental.pallas import tpu as pltpu
from jax.sharding import Mesh
from jax.sharding import PartitionSpec as P

ROPE = 64
LANES = 128
KV = ("kv_0", "kv_1", "kv_2")
REP_KV = ("rep", "kv_0", "kv_1", "kv_2")
MESH_ID = pl.DeviceIdType.MESH

softmax_scale = 192.0 ** (-0.5)
neg_floor = -1e30
f32 = jnp.float32
bf16 = jnp.bfloat16


def offset_of(j):
    return (j + 1) // 2 * (2 * (j % 2) - 1)


def ring_places(n):
    x, y, c = (lax.axis_index(axis) for axis in KV)

    def first_peer(d):
        return {"kv_0": (x + d * (1 - c) + n) % n, "kv_1": (y + d * c + n) % n, "kv_2": c}

    def second_peer(d):
        return {"kv_0": (x + d * c + n) % n, "kv_1": (y + d * (1 - c) + n) % n, "kv_2": c}

    partner = {"kv_0": x, "kv_1": y, "kv_2": 1 - c}
    return x, y, c, first_peer, second_peer, partner


def greet(peers):
    barrier = pltpu.get_barrier_semaphore()
    for peer in peers:
        pl.semaphore_signal(barrier, inc=1, device_id=peer, device_id_type=MESH_ID)
    pl.semaphore_wait(barrier, len(peers))


def send(src, dst, send_sem, recv_sem, peer):
    return pltpu.make_async_remote_copy(
        src_ref=src, dst_ref=dst, send_sem=send_sem, recv_sem=recv_sem, device_id=peer, device_id_type=MESH_ID
    )


def gather_kernel(
    n, q_ref, g_ref, other, pair_send, pair_recv, first_send, first_recv, right_send, right_recv, left_send, left_recv,
    share_send, share_recv
):
    x, y, c, first_peer, second_peer, partner = ring_places(n)
    half = n // 2
    block_tiles = g_ref.shape[2]
    greet([first_peer(offset_of(j)) for j in range(1, n)] + [second_peer(1), second_peer(-1), partner])
    swap = send(q_ref, other, pair_send, pair_recv, partner)
    swap.start()
    swap.wait()

    def place(a, b):
        return ((x + a * (1 - c) + b * c + 2 * n) % n) * n + (y + a * c + b * (1 - c) + 2 * n) % n

    mine = place(0, 0)
    query_count = q_ref.shape[0]
    latent_tiles = q_ref.shape[2] // LANES - 1
    tiles = []
    rotary = []
    for i in range(query_count):
        for t in range(latent_tiles + 1):
            cols = pl.ds(t * LANES, LANES)
            tile = q_ref[i, :, cols].astype(f32) + other[i, :, cols].astype(f32)
            (tiles if t < latent_tiles else rotary).append(tile)
    tiles.append(rotary[0] + pltpu.roll(rotary[1], ROPE, 1))
    tiles.append(rotary[2])
    for t in range(block_tiles):
        g_ref[c, mine, t] = jnp.where(c == 0, tiles[t], tiles[block_tiles + t]).astype(bf16)

    def share(block):
        ref = g_ref.at[c, block]
        send(ref, ref, share_send, share_recv, partner).start()

    def to_right(block, index):
        ref = g_ref.at[c, block]
        send(ref, ref, right_send, right_recv.at[index], second_peer(1)).start()

    def to_left(block, index):
        ref = g_ref.at[c, block]
        send(ref, ref, left_send, left_recv.at[index], second_peer(-1)).start()

    own = g_ref.at[c, mine]
    for j in range(1, n):
        send(own, own, first_send, first_recv.at[j], first_peer(offset_of(j))).start()
    to_right(mine, 0)
    to_left(mine, 0)
    share(mine)

    def first_step(j, _):
        block = place(-offset_of(j), 0)
        ref = g_ref.at[c, block]
        send(ref, ref, first_send, first_recv.at[j], partner).wait_recv()
        to_right(block, j)
        to_left(block, j)
        share(block)
        return 0

    lax.fori_loop(1, n, first_step, 0)

    def take_right(s, j, forward):
        block = place(-offset_of(j), -s)
        ref = g_ref.at[c, block]
        send(ref, ref, right_send, right_recv.at[(s - 1) * n + j], partner).wait_recv()
        if forward:
            to_right(block, s * n + j)
        share(block)

    def take_left(s, j, forward):
        block = place(-offset_of(j), s)
        ref = g_ref.at[c, block]
        send(ref, ref, left_send, left_recv.at[(s - 1) * n + j], partner).wait_recv()
        if forward:
            to_left(block, s * n + j)
        share(block)

    for s in range(1, half + 1):
        if s == half:

            def last_step(j, _):
                take_right(half, j, False)
                take_left(half, j + half, False)
                return 0

            lax.fori_loop(0, half, last_step, 0)
        elif s == half - 1:

            def low_step(j, _):
                take_right(half - 1, j, True)
                take_left(half - 1, j, False)
                return 0

            def high_step(j, _):
                take_right(half - 1, j, False)
                take_left(half - 1, j, True)
                return 0

            lax.fori_loop(0, half, low_step, 0)
            lax.fori_loop(half, n, high_step, 0)
        else:

            def mid_step(j, _, s=s):
                take_right(s, j, True)
                take_left(s, j, True)
                return 0

            lax.fori_loop(0, n, mid_step, 0)

    ring_blocks = n * (half - 1) + half
    some = g_ref.at[c, pl.ds(0, n - 1)]
    send(some, some, first_send, first_recv.at[0], partner).wait_send()
    some = g_ref.at[c, pl.ds(0, ring_blocks)]
    send(some, some, right_send, first_recv.at[0], partner).wait_send()
    send(some, some, left_send, first_recv.at[0], partner).wait_send()
    send(g_ref.at[c], g_ref.at[c], share_send, share_recv, partner).wait_send()
    send(g_ref.at[1 - c], g_ref.at[1 - c], share_send, share_recv, partner).wait_recv()


def gather_queries(q, n):
    query_count, requests, width = q.shape
    block_tiles = (query_count * (width // LANES - 1) + 2) // 2
    dma = pltpu.SemaphoreType.DMA
    return pl.pallas_call(
        functools.partial(gather_kernel, n),
        out_shape=jax.ShapeDtypeStruct((2, n * n, block_tiles, requests, LANES), bf16),
        in_specs=[pl.BlockSpec(memory_space=pltpu.VMEM)],
        out_specs=pl.BlockSpec(memory_space=pltpu.VMEM),
        scratch_shapes=[
            pltpu.VMEM(q.shape, bf16),
            dma, dma, dma, dma((n,)), dma, dma((n * n // 2,)), dma, dma((n * n // 2,)), dma, dma,
        ],
        compiler_params=pltpu.CompilerParams(collective_id=0, has_side_effects=True),
        name="gather_queries",
    )(q)


def attend_kernel(
    n, latent, g_ref, cache_ref, pages_ref, req, start, live, counts, part_ref, stat_ref, cache_v, cache_sem, sel, keys_v,
    q32, qr, acc, mrep, lrep, place, shift
):
    heads = n * n
    block_tiles, requests = g_ref.shape[2], g_ref.shape[3]
    span, slots = pages_ref.shape
    page_rows, width, page_count = cache_v.shape
    latent_tiles = latent // LANES
    query_count = part_ref.shape[2]
    rows = heads * query_count
    fetch = pltpu.make_async_copy(cache_ref, cache_v, cache_sem)
    fetch.start()

    def spread(h, _):
        def tile(t):
            return g_ref[t // block_tiles, h, t % block_tiles].astype(f32)

        for i in range(query_count):
            at = pl.ds(pl.multiple_of((h * query_count + i) * requests, requests), requests)
            for t in range(latent_tiles):
                q32[t, at, :] = tile(i * latent_tiles + t)
            rotary = tile(query_count * latent_tiles + i // 2)
            q32[latent_tiles, at, :] = pltpu.roll(rotary, ROPE, 1) if i % 2 else rotary
        return 0

    lax.fori_loop(0, heads, spread, 0)
    for r in range(requests):
        for t in range(latent_tiles + 1):
            qr[r, :, pl.ds(t * LANES, LANES)] = q32[t, pl.ds(r, rows, stride=requests), :].astype(bf16)

    acc[...] = jnp.zeros_like(acc)
    mrep[...] = jnp.full_like(mrep, neg_floor)
    lrep[...] = jnp.zeros_like(lrep)
    lane = lax.broadcasted_iota(jnp.int32, (rows, LANES), 1)
    place[...] = lane % span * page_rows + lane // span
    shift[...] = place[...] - lax.broadcasted_iota(jnp.int32, (rows, LANES), 0) % query_count
    page_lane = lax.broadcasted_iota(jnp.int32, (span, page_count), 1)
    for s in range(0, slots, 2):
        pair = [jnp.where(pages_ref[:, s + u : s + u + 1] == page_lane, 1.0, 0.0) for u in range(2)]
        sel[pl.ds(s * span, 2 * span), :] = jnp.concatenate(pair, axis=0).astype(bf16)
    fetch.wait()

    def pick(t, _):
        both = [
            lax.dot_general(
                sel[...], cache_v[2 * t + u], (((1,), (1,)), ((), ())), preferred_element_type=f32
            )
            for u in range(2)
        ]
        for s in range(slots):
            chunk = jnp.concatenate([one[s * span : (s + 1) * span] for one in both], axis=0)
            keys_v[s, pl.ds(pl.multiple_of(t * 2 * span, 2 * span), 2 * span), :] = chunk.astype(bf16)
        return 0

    lax.fori_loop(0, page_rows // 2, pick, 0)

    def slot_step(s, _):
        r = req[s]
        keys = keys_v[s]
        scores = (
            lax.dot_general(
                qr[r, :, :width], keys, (((1,), (1,)), ((), ())), preferred_element_type=f32
            )
            * softmax_scale
        )
        limit = (counts[r] - start[s]) * page_rows - (query_count - 1)
        visible = (place[...] < live[s] * page_rows) & (shift[...] < limit)
        slot_max = jnp.max(jnp.where(visible, scores, neg_floor), axis=1, keepdims=True)
        weights = jnp.exp(jnp.where(visible, scores - slot_max, neg_floor))
        slot_sum = jnp.sum(weights, axis=1, keepdims=True)
        slot_out = jnp.dot(weights.astype(bf16), keys[:, :latent], preferred_element_type=f32)
        at = pl.ds(r, rows, stride=requests)
        old = mrep[at, :]
        new = jnp.maximum(old, slot_max)
        kept = jnp.exp(old - new)
        added = jnp.exp(slot_max - new)
        mrep[at, :] = new
        lrep[at, :] = lrep[at, :] * kept + added * slot_sum
        for t in range(latent_tiles):
            acc[t, at, :] = acc[t, at, :] * kept + slot_out[:, t * LANES : (t + 1) * LANES] * added
        return 0

    lax.fori_loop(0, slots, slot_step, 0)

    def put(h, _):
        turned = h % n * n + h // n
        for i in range(query_count):
            at = pl.ds(pl.multiple_of((h * query_count + i) * requests, requests), requests)
            for t in range(latent_tiles):
                side = t * 2 // latent_tiles
                cols = pl.ds((t - side * latent_tiles // 2) * LANES, LANES)
                part_ref[side, h if side == 0 else turned, i, :, cols] = acc[t, at, :].astype(bf16)
        return 0

    lax.fori_loop(0, heads, put, 0)
    head_lane = lax.broadcasted_iota(jnp.int32, (heads, LANES), 1)
    stats = jnp.zeros((heads, LANES), f32)
    for i in range(query_count):
        for r in range(requests):
            at = pl.ds(i * requests + r, heads, stride=query_count * requests)
            stats = jnp.where(head_lane == i * requests + r, mrep[at, :], stats)
            stats = jnp.where(head_lane == (query_count + i) * requests + r, lrep[at, :], stats)
    stat_ref[0] = stats
    for a in range(n):
        stat_ref[1, pl.ds(a * n, n), :] = stat_ref[0, pl.ds(a, n, stride=n), :]


def attend(gathered, cache, pages, tables, n, query_count, latent):
    page_rows, key_width, page_count = cache.shape
    span, slots = pages.shape
    heads = n * n
    requests = gathered.shape[3]
    rows = heads * query_count
    vmem = pl.BlockSpec(memory_space=pltpu.VMEM)
    smem = pl.BlockSpec(memory_space=pltpu.SMEM)
    width = (latent // LANES + 1) * LANES
    return pl.pallas_call(
        functools.partial(attend_kernel, n, latent),
        out_shape=(
            jax.ShapeDtypeStruct((2, heads, query_count, requests, latent // 2), bf16),
            jax.ShapeDtypeStruct((2, heads, LANES), f32),
        ),
        in_specs=[vmem, pl.BlockSpec(memory_space=pl.ANY), vmem] + [smem] * 4,
        out_specs=(vmem, vmem),
        scratch_shapes=[
            pltpu.VMEM(cache.shape, bf16),
            pltpu.SemaphoreType.DMA,
            pltpu.VMEM((slots * span, page_count), bf16),
            pltpu.VMEM((slots, page_rows * span, key_width), bf16),
            pltpu.VMEM((width // LANES, rows * requests, LANES), f32),
            pltpu.VMEM((requests, rows, width), bf16),
            pltpu.VMEM((latent // LANES, rows * requests, LANES), f32),
            pltpu.VMEM((rows * requests, LANES), f32),
            pltpu.VMEM((rows * requests, LANES), f32),
            pltpu.VMEM((rows, LANES), jnp.int32),
            pltpu.VMEM((rows, LANES), jnp.int32),
        ],
        name="attend",
    )(gathered, cache, pages, *tables)


def combine_kernel(
    n, part_ref, stat_ref, out_ref, lse_ref, pair_part, pair_stat, f_mine, f_pair, chip_part, chip_stat, ring_part,
    ring_stat, f_ring, total, col_send_part, col_stat_send, col_part, col_stat, f_col, lse_send,
    sem_pair_stat, sem_pair_part, sem_stat_a, sem_part_a, sem_stat_b, sem_part_b, sem_lse
):
    x, y, c, first_peer, second_peer, partner = ring_places(n)
    a_here = x * (1 - c) + y * c
    b_here = y * (1 - c) + x * c
    _h, query_count, requests, cols = chip_part.shape[1:]
    m_lanes = query_count * requests
    greet(
        [first_peer(offset_of(j)) for j in range(1, n)] + [second_peer(offset_of(j)) for j in range(1, n)] + [partner]
    )
    order = list(range(n - 1, -1, -1))

    def a_at(d):
        return (a_here + d + n) % n

    def b_at(d):
        return (b_here + d + n) % n

    stat_swap = send(stat_ref.at[1 - c], pair_stat, sem_pair_stat.at[0], sem_pair_stat.at[1], partner)
    stat_swap.start()
    for j in order:
        a_pair = (b_here + offset_of(j) + n) % n
        send(
            part_ref.at[1 - c, a_pair], pair_part.at[a_pair], sem_pair_part.at[0, j], sem_pair_part.at[1, j], partner
        ).start()
    stat_swap.wait()

    lane8 = lax.broadcasted_iota(jnp.int32, (n, LANES), 1)
    lane16 = lax.broadcasted_iota(jnp.int32, (requests, LANES), 1)
    row16 = lax.broadcasted_iota(jnp.int32, (requests, LANES), 0)

    def column(row, base):
        picked = jnp.where(lane16 == row16 + base, jnp.broadcast_to(row, (requests, LANES)), 0.0)
        return jnp.sum(picked, axis=1, keepdims=True)

    def merged(all_stats):
        best = all_stats[0]
        for one in all_stats[1:]:
            best = jnp.maximum(best, one)
        factors = [jnp.exp(one - best) for one in all_stats]
        denom = 0.0
        for factor, one in zip(factors, all_stats):
            denom = denom + pltpu.roll(factor, m_lanes, 1) * one
        return factors, jnp.where(lane8 < m_lanes, best, denom)

    for a in range(n):
        factors, stats = merged([stat_ref[c, a], pair_stat[a]])
        f_mine[a] = factors[0]
        f_pair[a] = factors[1]
        chip_stat[a] = stats
    for j in order[:-1]:
        send(
            chip_stat.at[a_at(offset_of(j))], ring_stat.at[j], sem_stat_a.at[0, j], sem_stat_a.at[1, j],
            first_peer(offset_of(j)),
        ).start()
    ring_stat[0] = chip_stat[a_here]

    def pair_chunk(j, _):
        a_pair = (b_here + offset_of(j) + n) % n
        a = a_at(offset_of(j))
        send(
            part_ref.at[1 - c, a_pair], pair_part.at[a], sem_pair_part.at[0, j], sem_pair_part.at[1, j], partner
        ).wait()
        f_m = f_mine[a]
        f_p = f_pair[a]
        for b in range(n):
            for i in range(query_count):
                mine = part_ref[c, a, b, i].astype(f32) * column(f_m[b : b + 1], i * requests)
                theirs = pair_part[a, b, i].astype(f32) * column(f_p[b : b + 1], i * requests)
                chip_part[a, b, i] = (mine + theirs).astype(bf16)
        return a

    for j in order:
        a = pair_chunk(j, 0)
        if j:
            send(
                chip_part.at[a], ring_part.at[j], sem_part_a.at[0, j], sem_part_a.at[1, j], first_peer(offset_of(j))
            ).start()

    for j in range(1, n):
        send(
            chip_stat.at[a_here], ring_stat.at[j], sem_stat_a.at[0, j], sem_stat_a.at[1, j], first_peer(offset_of(j))
        ).wait()
    factors, stats = merged([ring_stat[j] for j in range(n)])
    for j in range(n):
        f_ring[j] = factors[j]
    col_stat_send[...] = stats
    for j in order[:-1]:
        send(
            col_stat_send, col_stat.at[j], sem_stat_b.at[0, j], sem_stat_b.at[1, j], second_peer(offset_of(j))
        ).start()
    col_stat[0] = stats
    for j in range(1, n):
        send(
            col_stat_send, col_stat.at[j], sem_stat_b.at[0, j], sem_stat_b.at[1, j], second_peer(offset_of(j))
        ).wait()
    factors, stats = merged([col_stat[j] for j in range(n)])
    for j in range(n):
        f_col[j] = factors[j]
    f_col[n] = stats
    lse = stats + jnp.log(pltpu.roll(jnp.where(lane8 < m_lanes, 1.0, stats), LANES - m_lanes, 1))
    lse_send[...] = lse
    lse_ref[a_here] = lse
    for j in range(1, n):
        send(
            lse_send, lse_ref.at[a_here], sem_lse.at[0, j], sem_lse.at[1, j], first_peer(offset_of(j))
        ).start()

    for j in range(n):
        if j:
            send(
                chip_part.at[a_here], ring_part.at[j], sem_part_a.at[0, j], sem_part_a.at[1, j],
                first_peer(offset_of(j)),
            ).wait()
        factor = f_ring[j]
        for b in range(n):
            for i in range(query_count):
                scale = column(factor[b : b + 1], i * requests)
                if j == 0:
                    total[b, i] = chip_part[a_here, b, i].astype(f32) * scale
                elif j < n - 1:
                    total[b, i] = total[b, i] + ring_part[j, b, i].astype(f32) * scale
                else:
                    col_send_part[b, i] = (total[b, i] + ring_part[j, b, i].astype(f32) * scale).astype(bf16)
    for j in order[:-1]:
        send(
            col_send_part.at[b_at(offset_of(j))], col_part.at[j], sem_part_b.at[0, j], sem_part_b.at[1, j],
            second_peer(offset_of(j)),
        ).start()
    sums = [0.0] * query_count
    for j in range(n):
        if j:
            send(
                col_send_part.at[b_here], col_part.at[j], sem_part_b.at[0, j], sem_part_b.at[1, j],
                second_peer(offset_of(j)),
            ).wait()
        row = f_col[j, pl.ds(b_here, 1), :]
        for i in range(query_count):
            block = col_send_part[b_here, i] if j == 0 else col_part[j, i]
            sums[i] = sums[i] + block.astype(f32) * column(row, i * requests)
    row = f_col[n, pl.ds(b_here, 1), :]
    for i in range(query_count):
        out_ref[i] = (sums[i] / column(row, m_lanes + i * requests)).astype(bf16)
    for j in range(1, n):
        a_from = a_at(-offset_of(j))
        send(
            lse_send, lse_ref.at[a_from], sem_lse.at[0, j], sem_lse.at[1, j], first_peer(offset_of(j))
        ).wait()


def combine(part, stat, n):
    _two, heads, query_count, requests, cols = part.shape
    part = part.reshape(2, n, n, query_count, requests, cols)
    stat = stat.reshape(2, n, n, LANES)
    vmem = pl.BlockSpec(memory_space=pltpu.VMEM)
    dma = pltpu.SemaphoreType.DMA
    block = (n, n, query_count, requests, cols)
    one = (n, query_count, requests, cols)
    return pl.pallas_call(
        functools.partial(combine_kernel, n),
        out_shape=(
            jax.ShapeDtypeStruct((query_count, requests, cols), bf16),
            jax.ShapeDtypeStruct((n, n, LANES), f32),
        ),
        in_specs=[vmem, vmem],
        out_specs=(vmem, vmem),
        scratch_shapes=[
            pltpu.VMEM(block, bf16),
            pltpu.VMEM((n, n, LANES), f32),
            pltpu.VMEM((n, n, LANES), f32),
            pltpu.VMEM((n, n, LANES), f32),
            pltpu.VMEM(block, bf16),
            pltpu.VMEM((n, n, LANES), f32),
            pltpu.VMEM(block, bf16),
            pltpu.VMEM((n, n, LANES), f32),
            pltpu.VMEM((n, n, LANES), f32),
            pltpu.VMEM(one, f32),
            pltpu.VMEM(one, bf16),
            pltpu.VMEM((n, LANES), f32),
            pltpu.VMEM(one, bf16),
            pltpu.VMEM((n, n, LANES), f32),
            pltpu.VMEM((n + 1, n, LANES), f32),
            pltpu.VMEM((n, LANES), f32),
            dma((2,)),
            dma((2, n)), dma((2, n)), dma((2, n)), dma((2, n)), dma((2, n)), dma((2, n)),
        ],
        compiler_params=pltpu.CompilerParams(collective_id=1, has_side_effects=True),
        name="combine",
    )(part, stat)


def per_device(n, queries, cache, page_counts, slot_request, slot_start, slot_live, slot_pages):
    requests, query_count, share = queries.shape
    width = cache.shape[2]
    latent = width - ROPE
    core = lax.axis_index(KV[2])
    turned = jnp.transpose(queries, (1, 0, 2))
    padded = (latent // LANES + 1) * LANES
    low = jnp.pad(turned, ((0, 0), (0, 0), (0, padded - share)))
    high = jnp.pad(turned, ((0, 0), (0, 0), (share, padded - 2 * share)))
    q = jnp.where(core == 0, low, high)
    gathered = gather_queries(q, n)
    tables = (slot_request, slot_start, slot_live, page_counts)
    turned_cache = jnp.transpose(cache, (1, 2, 0))
    part, stat = attend(gathered, turned_cache, slot_pages.T, tables, n, query_count, latent)
    out, lse = combine(part, stat, n)
    attended = jnp.transpose(out, (1, 0, 2))
    lse = jnp.where(core == 0, lse, jnp.swapaxes(lse, 0, 1))
    lse = lse.reshape(n * n, LANES)[:, : query_count * requests].reshape(n * n, query_count, requests)
    return attended, jnp.transpose(lse, (2, 1, 0))


def solution(mesh):
    n = round((mesh.shape["kv"] // 2) ** 0.5)
    split = Mesh(mesh.devices.reshape(mesh.shape["rep"], n, n, 2), REP_KV)
    placed = (
        P("rep", None, KV),
        P(REP_KV, None, None),
        P("rep"),
        P(REP_KV),
        P(REP_KV),
        P(REP_KV),
        P(REP_KV, None),
    )
    return jax.shard_map(
        functools.partial(per_device, n),
        mesh=split,
        in_specs=placed,
        out_specs=(P("rep", None, KV), P("rep", None, None)),
        check_vma=False,
    )
```

```python
import functools
from types import SimpleNamespace

import jax
import jax.numpy as jnp
from jax import lax
from jax.experimental import pallas as pl
from jax.experimental.pallas import tpu as pltpu
from jax.sharding import Mesh
from jax.sharding import PartitionSpec as P

ROPE = 64
LANES = 128
KV = ("kv_0", "kv_1", "kv_2")
REP_KV = ("rep", "kv_0", "kv_1", "kv_2")
MESH_ID = pl.DeviceIdType.MESH

softmax_scale = 192.0 ** (-0.5)
neg_floor = -1e30
f32 = jnp.float32
bf16 = jnp.bfloat16


def offset_of(j):
    return (j + 1) // 2 * (2 * (j % 2) - 1)


def ring_places(n):
    x, y, c = (lax.axis_index(axis) for axis in KV)

    def first_peer(d):
        return {"kv_0": (x + d * (1 - c) + n) % n, "kv_1": (y + d * c + n) % n, "kv_2": c}

    def second_peer(d):
        return {"kv_0": (x + d * c + n) % n, "kv_1": (y + d * (1 - c) + n) % n, "kv_2": c}

    partner = {"kv_0": x, "kv_1": y, "kv_2": 1 - c}
    return x, y, c, first_peer, second_peer, partner


def greet(peers):
    barrier = pltpu.get_barrier_semaphore()
    for peer in peers:
        pl.semaphore_signal(barrier, inc=1, device_id=peer, device_id_type=MESH_ID)
    pl.semaphore_wait(barrier, len(peers))


def send(src, dst, send_sem, recv_sem, peer):
    return pltpu.make_async_remote_copy(
        src_ref=src, dst_ref=dst, send_sem=send_sem, recv_sem=recv_sem, device_id=peer, device_id_type=MESH_ID
    )


def decode_kernel(n, latent, names, *refs):
    v = SimpleNamespace(**dict(zip(names, refs)))
    x, y, c, first_peer, second_peer, partner = ring_places(n)
    fetch = pltpu.make_async_copy(v.cache, v.cache_v, v.cache_sem)
    fetch.start()
    greet(
        [first_peer(offset_of(j)) for j in range(1, n)] + [second_peer(offset_of(j)) for j in range(1, n)] + [partner]
    )
    gather_part(n, v, x, y, c, first_peer, second_peer, partner, fetch)
    attend_part(n, latent, v, c)
    combine_part(n, v, x, y, c, first_peer, second_peer, partner)


def attention_tables(n, v):
    slots = v.req.shape[0]
    requests = v.counts.shape[0]
    requested = [v.req[s] for s in range(slots)]

    def find_before(s, _):
        mine = v.req[s]
        found = slots
        for t in range(slots):
            found = jnp.where((requested[t] == mine) & (t < s), t, found)
        v.before[s] = found
        return 0

    def find_last(r, _):
        found = slots
        for t in range(slots):
            found = jnp.where(requested[t] == r, t, found)
        v.last[r] = found
        return 0

    lax.fori_loop(0, slots, find_before, 0)
    lax.fori_loop(0, requests, find_last, 0)


def attention_constants(n, v):
    span, slots = v.pages.shape
    page_rows, _width, page_count = v.cache_v.shape
    requests = v.counts.shape[0]
    heads = n * n
    rows = v.place.shape[0]
    group = min(requests, heads)
    size = requests * group
    lane = lax.broadcasted_iota(jnp.int32, (rows, LANES), 1)
    v.place[...] = lane % span * page_rows + lane // span
    v.shift[...] = v.place[...] - lax.broadcasted_iota(jnp.int32, (rows, LANES), 0) // heads
    turn_row = lax.broadcasted_iota(jnp.int32, (size, size), 0)
    turn_col = lax.broadcasted_iota(jnp.int32, (size, size), 1)
    from_heads = jnp.where(turn_col == turn_row % group * requests + turn_row // group, 1.0, 0.0)
    v.turn[0] = from_heads.astype(bf16)
    to_heads = jnp.where(turn_row == turn_col % group * requests + turn_col // group, 1.0, 0.0)
    v.turn[1] = to_heads.astype(bf16)
    page_lane = lax.broadcasted_iota(jnp.int32, (span, page_count), 1)
    for s in range(0, slots, 2):
        pair = [jnp.where(v.pages[:, s + u : s + u + 1] == page_lane, 1.0, 0.0) for u in range(2)]
        v.sel[pl.ds(s * span, 2 * span), :] = jnp.concatenate(pair, axis=0).astype(bf16)
    v.acc[slots] = jnp.zeros(v.acc.shape[1:], f32)
    v.mrep[slots] = jnp.full(v.mrep.shape[1:], neg_floor, f32)
    v.lrep[slots] = jnp.zeros(v.lrep.shape[1:], f32)


def pick_rows(v, t):
    span, slots = v.pages.shape
    both = [
        lax.dot_general(v.sel[...], v.cache_v[2 * t + u], (((1,), (1,)), ((), ())), preferred_element_type=f32)
        for u in range(2)
    ]
    for s in range(slots):
        chunk = jnp.concatenate([one[s * span : (s + 1) * span] for one in both], axis=0)
        v.keys_v[s, pl.ds(pl.multiple_of(t * 2 * span, 2 * span), 2 * span), :] = chunk.astype(bf16)


def gather_part(n, v, x, y, c, first_peer, second_peer, partner, fetch):
    half = n // 2
    block_tiles = v.gathered.shape[2]
    g_ref, q_ref, other = v.gathered, v.q, v.other
    swap = send(q_ref, other, v.pair_send, v.pair_recv, partner)
    swap.start()
    swap.wait()

    def place(a, b):
        return ((x + a * (1 - c) + b * c + 2 * n) % n) * n + (y + a * c + b * (1 - c) + 2 * n) % n

    mine = place(0, 0)
    query_count, requests, held = q_ref.shape
    lane = lax.broadcasted_iota(jnp.int32, (requests, LANES), 1)
    tail = held % LANES
    pad = jnp.zeros((requests, LANES - tail), f32)
    tiles = []
    rotary = []
    for i in range(query_count):
        here = q_ref[i].astype(f32)
        there = other[i].astype(f32)
        low = jnp.concatenate([jnp.where(c == 0, here, there), pad], axis=1)
        high = jnp.concatenate([jnp.where(c == 0, there, here), pad], axis=1)
        full = held // LANES
        low = [low[:, t * LANES : (t + 1) * LANES] for t in range(full + 1)]
        high = [pltpu.roll(high[:, t * LANES : (t + 1) * LANES], tail, 1) for t in range(full + 1)]
        tiles += low[:full]
        left = low[full]
        for t in range(full):
            tiles.append(jnp.where(lane < tail, left, high[t]))
            left = high[t]
        rotary.append(jnp.where(lane < tail, left, jnp.where(lane < 2 * tail, high[full], 0.0)))
    tiles.append(rotary[0] + pltpu.roll(rotary[1], ROPE, 1))
    tiles.append(rotary[2])
    for t in range(block_tiles):
        g_ref[c, mine, t] = jnp.where(c == 0, tiles[t], tiles[block_tiles + t]).astype(bf16)

    def share(block):
        ref = g_ref.at[c, block]
        send(ref, ref, v.share_send, v.share_recv, partner).start()

    def to_right(block, index):
        ref = g_ref.at[c, block]
        send(ref, ref, v.right_send, v.right_recv.at[index], second_peer(1)).start()

    def to_left(block, index):
        ref = g_ref.at[c, block]
        send(ref, ref, v.left_send, v.left_recv.at[index], second_peer(-1)).start()

    own = g_ref.at[c, mine]
    for j in range(1, n):
        send(own, own, v.first_send, v.first_recv.at[j], first_peer(offset_of(j))).start()
    to_right(mine, 0)
    to_left(mine, 0)
    share(mine)

    def first_step(j, _):
        block = place(-offset_of(j), 0)
        ref = g_ref.at[c, block]
        send(ref, ref, v.first_send, v.first_recv.at[j], partner).wait_recv()
        to_right(block, j)
        to_left(block, j)
        share(block)
        pick_rows(v, j - 1)
        return 0

    attention_tables(n, v)
    attention_constants(n, v)
    fetch.wait()
    lax.fori_loop(1, n, first_step, 0)
    for t in range(n - 1, v.cache_v.shape[0] // 2):
        pick_rows(v, t)

    def take_right(s, j, forward):
        block = place(-offset_of(j), -s)
        ref = g_ref.at[c, block]
        send(ref, ref, v.right_send, v.right_recv.at[(s - 1) * n + j], partner).wait_recv()
        if forward:
            to_right(block, s * n + j)
        share(block)

    def take_left(s, j, forward):
        block = place(-offset_of(j), s)
        ref = g_ref.at[c, block]
        send(ref, ref, v.left_send, v.left_recv.at[(s - 1) * n + j], partner).wait_recv()
        if forward:
            to_left(block, s * n + j)
        share(block)

    for s in range(1, half + 1):
        if s == half:

            def last_step(j, _):
                take_right(half, j, False)
                take_left(half, j + half, False)
                return 0

            lax.fori_loop(0, half, last_step, 0)
        elif s == half - 1:

            def low_step(j, _):
                take_right(half - 1, j, True)
                take_left(half - 1, j, False)
                return 0

            def high_step(j, _):
                take_right(half - 1, j, False)
                take_left(half - 1, j, True)
                return 0

            lax.fori_loop(0, half, low_step, 0)
            lax.fori_loop(half, n, high_step, 0)
        else:

            def mid_step(j, _, s=s):
                take_right(s, j, True)
                take_left(s, j, True)
                return 0

            lax.fori_loop(0, n, mid_step, 0)

    ring_blocks = n * (half - 1) + half
    some = g_ref.at[c, pl.ds(0, n - 1)]
    send(some, some, v.first_send, v.first_recv.at[0], partner).wait_send()
    some = g_ref.at[c, pl.ds(0, ring_blocks)]
    send(some, some, v.right_send, v.first_recv.at[0], partner).wait_send()
    send(some, some, v.left_send, v.first_recv.at[0], partner).wait_send()
    send(g_ref.at[c], g_ref.at[c], v.share_send, v.share_recv, partner).wait_send()
    send(g_ref.at[1 - c], g_ref.at[1 - c], v.share_send, v.share_recv, partner).wait_recv()


def attend_part(n, latent, v, c):
    heads = n * n
    block_tiles, requests = v.gathered.shape[2], v.gathered.shape[3]
    span, slots = v.pages.shape
    page_rows, width, page_count = v.cache_v.shape
    latent_tiles = latent // LANES
    query_count = v.q.shape[0]
    group = min(requests, heads)
    unroll = min(slots, 4)

    def spread(block, _):
        h = block * group
        for i in range(query_count):
            base = pl.multiple_of(i * heads + h, group)

            def turned(t):
                stack = jnp.concatenate(
                    [v.gathered[t // block_tiles, h + u, t % block_tiles] for u in range(group)], axis=0
                )
                return jnp.dot(v.turn[0], stack, preferred_element_type=f32)

            def keep(t, tile):
                for r in range(requests):
                    v.qr[r, pl.ds(base, group), pl.ds(t * LANES, LANES)] = tile[r * group : (r + 1) * group].astype(bf16)

            for t in range(latent_tiles):
                keep(t, turned(i * latent_tiles + t))
            rotary = turned(query_count * latent_tiles + i // 2)
            keep(latent_tiles, pltpu.roll(rotary, ROPE, 1) if i % 2 else rotary)
        return 0

    lax.fori_loop(0, heads // group, spread, 0)

    def slot_step(g, _):
        held = []
        for u in range(unroll):
            s = g * unroll + u
            r = v.req[s]
            scores = (
                lax.dot_general(
                    v.qr[r, :, :width], v.keys_v[s], (((1,), (1,)), ((), ())), preferred_element_type=f32
                )
                * softmax_scale
            )
            limit = (v.counts[r] - v.start[s]) * page_rows - (query_count - 1)
            visible = (v.place[...] < v.live[s] * page_rows) & (v.shift[...] < limit)
            slot_max = jnp.max(jnp.where(visible, scores, neg_floor), axis=1, keepdims=True)
            weights = jnp.exp(jnp.where(visible, scores - slot_max, neg_floor))
            slot_sum = jnp.sum(weights, axis=1, keepdims=True)
            held.append((weights.astype(bf16), slot_max, slot_sum))
        for u in range(unroll):
            s = g * unroll + u
            p = v.before[s]
            weights, slot_max, slot_sum = held[u]
            old = v.mrep[p]
            new = jnp.maximum(old, slot_max)
            kept = jnp.exp(old - new)
            added = jnp.exp(slot_max - new)
            v.mrep[s] = new
            v.lrep[s] = v.lrep[p] * kept + added * slot_sum
            for t in range(0, latent_tiles, 2):
                out = jnp.dot(weights, v.keys_v[s, :, t * LANES : (t + 2) * LANES], preferred_element_type=f32)
                for w in range(2):
                    v.acc[s, t + w] = v.acc[p, t + w] * kept + out[:, w * LANES : (w + 1) * LANES] * added
        return 0

    lax.fori_loop(0, slots // unroll, slot_step, 0)
    last = [v.last[r] for r in range(requests)]
    head_lane = lax.broadcasted_iota(jnp.int32, (heads, LANES), 1)
    stats = jnp.zeros((heads, LANES), f32)
    for i in range(query_count):
        for r in range(requests):
            at = pl.ds(i * heads, heads)
            stats = jnp.where(head_lane == i * requests + r, v.mrep[last[r], at, :], stats)
            stats = jnp.where(head_lane == (query_count + i) * requests + r, v.lrep[last[r], at, :], stats)
    v.flat[...] = stats
    for a in range(n):
        v.stat[0, a] = v.flat[pl.ds(a * n, n), :]
        v.stat[1, a] = v.flat[pl.ds(a, n, stride=n), :]


def put_side(n, latent, v, side):
    heads = n * n
    requests = v.counts.shape[0]
    query_count = v.q.shape[0]
    group = min(requests, heads)
    side_tiles = latent // LANES // 2
    last = [v.last[r] for r in range(requests)]

    def put(block, _):
        h = block * group
        for i in range(query_count):
            base = pl.multiple_of(i * heads + h, group)
            for t in range(side_tiles):
                tile = side * side_tiles + t
                stack = jnp.concatenate(
                    [v.acc[last[r], tile, pl.ds(base, group), :] for r in range(requests)], axis=0
                )
                flat = jnp.dot(v.turn[1], stack.astype(bf16), preferred_element_type=f32).astype(bf16)
                for u in range(group):
                    high, low = (h + u) // n, (h + u) % n
                    a = high * (1 - side) + low * side
                    b = low * (1 - side) + high * side
                    v.part[side, a, b, i, :, pl.ds(t * LANES, LANES)] = flat[u * requests : (u + 1) * requests]
        return 0

    lax.fori_loop(0, heads // group, put, 0)


def combine_part(n, v, x, y, c, first_peer, second_peer, partner):
    a_here = x * (1 - c) + y * c
    b_here = y * (1 - c) + x * c
    _h, query_count, requests, cols = v.chip_part.shape[1:]
    m_lanes = query_count * requests
    order = list(range(n - 1, -1, -1))

    def a_at(d):
        return (a_here + d + n) % n

    def b_at(d):
        return (b_here + d + n) % n

    stat_swap = send(v.stat.at[1 - c], v.pair_stat, v.sem_pair_stat.at[0], v.sem_pair_stat.at[1], partner)
    stat_swap.start()
    put_side(n, 2 * cols, v, 1 - c)
    for j in order:
        a_pair = (b_here + offset_of(j) + n) % n
        send(
            v.part.at[1 - c, a_pair], v.pair_part.at[a_pair], v.sem_pair_part.at[0, j], v.sem_pair_part.at[1, j], partner
        ).start()
    put_side(n, 2 * cols, v, c)
    stat_swap.wait()

    lane8 = lax.broadcasted_iota(jnp.int32, (n, LANES), 1)
    lane16 = lax.broadcasted_iota(jnp.int32, (requests, LANES), 1)
    row16 = lax.broadcasted_iota(jnp.int32, (requests, LANES), 0)

    def column(row, base):
        picked = jnp.where(lane16 == row16 + base, jnp.broadcast_to(row, (requests, LANES)), 0.0)
        return jnp.sum(picked, axis=1, keepdims=True)

    def merged(all_stats):
        best = all_stats[0]
        for one in all_stats[1:]:
            best = jnp.maximum(best, one)
        factors = [jnp.exp(one - best) for one in all_stats]
        denom = 0.0
        for factor, one in zip(factors, all_stats):
            denom = denom + pltpu.roll(factor, m_lanes, 1) * one
        return factors, jnp.where(lane8 < m_lanes, best, denom)

    for a in range(n):
        factors, stats = merged([v.stat[c, a], v.pair_stat[a]])
        v.f_mine[a] = factors[0]
        v.f_pair[a] = factors[1]
        v.chip_stat[a] = stats
    for j in order[:-1]:
        send(
            v.chip_stat.at[a_at(offset_of(j))], v.ring_stat.at[j], v.sem_stat_a.at[0, j], v.sem_stat_a.at[1, j],
            first_peer(offset_of(j)),
        ).start()
    v.ring_stat[0] = v.chip_stat[a_here]

    def pair_chunk(j, _):
        a_pair = (b_here + offset_of(j) + n) % n
        a = a_at(offset_of(j))
        send(
            v.part.at[1 - c, a_pair], v.pair_part.at[a], v.sem_pair_part.at[0, j], v.sem_pair_part.at[1, j], partner
        ).wait()
        f_m = v.f_mine[a]
        f_p = v.f_pair[a]
        for b in range(n):
            for i in range(query_count):
                mine = v.part[c, a, b, i].astype(f32) * column(f_m[b : b + 1], i * requests)
                theirs = v.pair_part[a, b, i].astype(f32) * column(f_p[b : b + 1], i * requests)
                v.chip_part[a, b, i] = (mine + theirs).astype(bf16)
        return a

    for j in order:
        a = pair_chunk(j, 0)
        if j:
            send(
                v.chip_part.at[a], v.ring_part.at[j], v.sem_part_a.at[0, j], v.sem_part_a.at[1, j], first_peer(offset_of(j))
            ).start()

    for j in range(1, n):
        send(
            v.chip_stat.at[a_here], v.ring_stat.at[j], v.sem_stat_a.at[0, j], v.sem_stat_a.at[1, j], first_peer(offset_of(j))
        ).wait()
    factors, stats = merged([v.ring_stat[j] for j in range(n)])
    for j in range(n):
        v.f_ring[j] = factors[j]
    v.col_stat_send[...] = stats
    for j in order[:-1]:
        send(
            v.col_stat_send, v.col_stat.at[j], v.sem_stat_b.at[0, j], v.sem_stat_b.at[1, j], second_peer(offset_of(j))
        ).start()
    v.col_stat[0] = stats
    for j in range(1, n):
        send(
            v.col_stat_send, v.col_stat.at[j], v.sem_stat_b.at[0, j], v.sem_stat_b.at[1, j], second_peer(offset_of(j))
        ).wait()
    factors, stats = merged([v.col_stat[j] for j in range(n)])
    for j in range(n):
        v.f_col[j] = factors[j]
    v.f_col[n] = stats
    lse = stats + jnp.log(pltpu.roll(jnp.where(lane8 < m_lanes, 1.0, stats), LANES - m_lanes, 1))
    v.lse_send[...] = lse
    v.lse_all[a_here] = lse
    for j in range(1, n):
        send(
            v.lse_send, v.lse_all.at[a_here], v.sem_lse.at[0, j], v.sem_lse.at[1, j], first_peer(offset_of(j))
        ).start()

    for j in range(n):
        if j:
            send(
                v.chip_part.at[a_here], v.ring_part.at[j], v.sem_part_a.at[0, j], v.sem_part_a.at[1, j],
                first_peer(offset_of(j)),
            ).wait()
        factor = v.f_ring[j]
        for b in range(n):
            for i in range(query_count):
                scale = column(factor[b : b + 1], i * requests)
                if j == 0:
                    v.total[b, i] = v.chip_part[a_here, b, i].astype(f32) * scale
                elif j < n - 1:
                    v.total[b, i] = v.total[b, i] + v.ring_part[j, b, i].astype(f32) * scale
                else:
                    v.col_send_part[b, i] = (v.total[b, i] + v.ring_part[j, b, i].astype(f32) * scale).astype(bf16)
    for j in order[:-1]:
        send(
            v.col_send_part.at[b_at(offset_of(j))], v.col_part.at[j], v.sem_part_b.at[0, j], v.sem_part_b.at[1, j],
            second_peer(offset_of(j)),
        ).start()
    sums = [0.0] * query_count
    for j in range(n):
        if j:
            send(
                v.col_send_part.at[b_here], v.col_part.at[j], v.sem_part_b.at[0, j], v.sem_part_b.at[1, j],
                second_peer(offset_of(j)),
            ).wait()
        row = v.f_col[j, pl.ds(b_here, 1), :]
        for i in range(query_count):
            block = v.col_send_part[b_here, i] if j == 0 else v.col_part[j, i]
            sums[i] = sums[i] + block.astype(f32) * column(row, i * requests)
    row = v.f_col[n, pl.ds(b_here, 1), :]
    for i in range(query_count):
        v.out[i] = (sums[i] / column(row, m_lanes + i * requests)).astype(bf16)
    for j in range(1, n):
        a_from = a_at(-offset_of(j))
        send(
            v.lse_send, v.lse_all.at[a_from], v.sem_lse.at[0, j], v.sem_lse.at[1, j], first_peer(offset_of(j))
        ).wait()
    heads = n * n
    for a in range(n):
        v.flat[pl.ds(a * n, n), :] = v.lse_all[a]
    turned = jnp.concatenate([v.flat[pl.ds(a, n, stride=n), :] for a in range(n)], axis=0)
    lse = jnp.where(c == 0, v.flat[...], turned)
    if heads < LANES:
        lse = jnp.concatenate([lse, jnp.zeros((LANES - heads, LANES), f32)], axis=0)
    lse = jnp.transpose(lse)
    for i in range(query_count):
        v.lse[i] = lse[i * requests : (i + 1) * requests, :heads]


def decode(q, cache, pages, tables, n, latent):
    query_count, requests, _held = q.shape
    page_rows, width, page_count = cache.shape
    span, slots = pages.shape
    heads = n * n
    rows = heads * query_count
    cols = latent // 2
    tiles = latent // LANES
    block_tiles = (query_count * tiles + 2) // 2
    size = requests * min(requests, heads)
    dma = pltpu.SemaphoreType.DMA
    vmem = pl.BlockSpec(memory_space=pltpu.VMEM)
    smem = pl.BlockSpec(memory_space=pltpu.SMEM)
    block = (n, n, query_count, requests, cols)
    one = (n, query_count, requests, cols)
    scratch = dict(
        cache_v=pltpu.VMEM(cache.shape, bf16),
        cache_sem=dma,
        gathered=pltpu.VMEM((2, heads, block_tiles, requests, LANES), bf16),
        other=pltpu.VMEM(q.shape, bf16),
        before=pltpu.SMEM((slots,), jnp.int32),
        last=pltpu.SMEM((requests,), jnp.int32),
        pair_send=dma, pair_recv=dma, first_send=dma, first_recv=dma((n,)), right_send=dma,
        right_recv=dma((n * n // 2,)), left_send=dma, left_recv=dma((n * n // 2,)), share_send=dma, share_recv=dma,
        sel=pltpu.VMEM((slots * span, page_count), bf16),
        keys_v=pltpu.VMEM((slots, page_rows * span, width), bf16),
        qr=pltpu.VMEM((requests, rows, (tiles + 1) * LANES), bf16),
        acc=pltpu.VMEM((slots + 1, tiles, rows, LANES), f32),
        mrep=pltpu.VMEM((slots + 1, rows, LANES), f32),
        lrep=pltpu.VMEM((slots + 1, rows, LANES), f32),
        turn=pltpu.VMEM((2, size, size), bf16),
        place=pltpu.VMEM((rows, LANES), jnp.int32),
        shift=pltpu.VMEM((rows, LANES), jnp.int32),
        flat=pltpu.VMEM((heads, LANES), f32),
        part=pltpu.VMEM((2,) + block, bf16),
        stat=pltpu.VMEM((2, n, n, LANES), f32),
        pair_part=pltpu.VMEM(block, bf16),
        pair_stat=pltpu.VMEM((n, n, LANES), f32),
        f_mine=pltpu.VMEM((n, n, LANES), f32),
        f_pair=pltpu.VMEM((n, n, LANES), f32),
        chip_part=pltpu.VMEM(block, bf16),
        chip_stat=pltpu.VMEM((n, n, LANES), f32),
        ring_part=pltpu.VMEM(block, bf16),
        ring_stat=pltpu.VMEM((n, n, LANES), f32),
        f_ring=pltpu.VMEM((n, n, LANES), f32),
        total=pltpu.VMEM(one, f32),
        col_send_part=pltpu.VMEM(one, bf16),
        col_stat_send=pltpu.VMEM((n, LANES), f32),
        col_part=pltpu.VMEM(one, bf16),
        col_stat=pltpu.VMEM((n, n, LANES), f32),
        f_col=pltpu.VMEM((n + 1, n, LANES), f32),
        lse_send=pltpu.VMEM((n, LANES), f32),
        lse_all=pltpu.VMEM((n, n, LANES), f32),
        sem_pair_stat=dma((2,)),
        sem_pair_part=dma((2, n)), sem_stat_a=dma((2, n)), sem_part_a=dma((2, n)), sem_stat_b=dma((2, n)),
        sem_part_b=dma((2, n)), sem_lse=dma((2, n)),
    )
    names = ["q", "cache", "pages", "req", "start", "live", "counts", "out", "lse"] + list(scratch)
    return pl.pallas_call(
        functools.partial(decode_kernel, n, latent, names),
        out_shape=(
            jax.ShapeDtypeStruct((query_count, requests, cols), bf16),
            jax.ShapeDtypeStruct((query_count, requests, heads), f32),
        ),
        in_specs=[vmem, pl.BlockSpec(memory_space=pl.ANY), vmem] + [smem] * 4,
        out_specs=(vmem, vmem),
        scratch_shapes=list(scratch.values()),
        compiler_params=pltpu.CompilerParams(
            collective_id=0, has_side_effects=True, vmem_limit_bytes=62 * 2**20
        ),
        name="decode",
    )(q, cache, pages, *tables)


def per_device(n, queries, cache, page_counts, slot_request, slot_start, slot_live, slot_pages):
    latent = cache.shape[2] - ROPE
    tables = (slot_request, slot_start, slot_live, page_counts)
    out, lse = decode(
        jnp.transpose(queries, (1, 0, 2)), jnp.transpose(cache, (1, 2, 0)), slot_pages.T, tables, n, latent
    )
    return jnp.transpose(out, (1, 0, 2)), jnp.transpose(lse, (1, 0, 2))


def solution(mesh):
    n = round((mesh.shape["kv"] // 2) ** 0.5)
    split = Mesh(mesh.devices.reshape(mesh.shape["rep"], n, n, 2), REP_KV)
    placed = (
        P("rep", None, KV),
        P(REP_KV, None, None),
        P("rep"),
        P(REP_KV),
        P(REP_KV),
        P(REP_KV),
        P(REP_KV, None),
    )
    return jax.shard_map(
        functools.partial(per_device, n),
        mesh=split,
        in_specs=placed,
        out_specs=(P("rep", None, KV), P("rep", None, None)),
        check_vma=False,
    )
```

```python
import functools
from types import SimpleNamespace

import jax
import jax.numpy as jnp
from jax import lax
from jax.experimental import pallas as pl
from jax.experimental.pallas import tpu as pltpu
from jax.sharding import Mesh
from jax.sharding import PartitionSpec as P

ROPE = 64
LANES = 128
KV = ("kv_0", "kv_1", "kv_2")
REP_KV = ("rep", "kv_0", "kv_1", "kv_2")
MESH_ID = pl.DeviceIdType.MESH

softmax_scale = 192.0 ** (-0.5)
neg_floor = -1e30
f32 = jnp.float32
bf16 = jnp.bfloat16


def offset_of(j):
    return (j + 1) // 2 * (2 * (j % 2) - 1)


def ring_places(n):
    x, y, c = (lax.axis_index(axis) for axis in KV)

    def first_peer(d):
        return {"kv_0": (x + d * (1 - c) + n) % n, "kv_1": (y + d * c + n) % n, "kv_2": c}

    def second_peer(d):
        return {"kv_0": (x + d * c + n) % n, "kv_1": (y + d * (1 - c) + n) % n, "kv_2": c}

    partner = {"kv_0": x, "kv_1": y, "kv_2": 1 - c}
    return x, y, c, first_peer, second_peer, partner


def greet(peers):
    barrier = pltpu.get_barrier_semaphore()
    for peer in peers:
        pl.semaphore_signal(barrier, inc=1, device_id=peer, device_id_type=MESH_ID)
    pl.semaphore_wait(barrier, len(peers))


def send(src, dst, send_sem, recv_sem, peer):
    return pltpu.make_async_remote_copy(
        src_ref=src, dst_ref=dst, send_sem=send_sem, recv_sem=recv_sem, device_id=peer, device_id_type=MESH_ID
    )


def decode_kernel(n, latent, names, *refs):
    v = SimpleNamespace(**dict(zip(names, refs)))
    x, y, c, first_peer, second_peer, partner = ring_places(n)
    fetch = pltpu.make_async_copy(v.cache, v.cache_v, v.cache_sem)
    fetch.start()
    greet(
        [first_peer(offset_of(j)) for j in range(1, n)] + [second_peer(offset_of(j)) for j in range(1, n)] + [partner]
    )
    gather_part(n, v, x, y, c, first_peer, second_peer, partner, fetch)
    attend_part(n, latent, v, c)
    combine_part(n, v, x, y, c, first_peer, second_peer, partner)
    gather_sent(n, v, c, partner)


def attention_tables(n, v):
    slots = v.req.shape[0]
    requests = v.counts.shape[0]
    requested = [v.req[s] for s in range(slots)]

    def find_before(s, _):
        mine = v.req[s]
        found = slots
        for t in range(slots):
            found = jnp.where((requested[t] == mine) & (t < s), t, found)
        v.before[s] = found
        return 0

    def find_last(r, _):
        found = slots
        for t in range(slots):
            found = jnp.where(requested[t] == r, t, found)
        v.last[r] = found
        return 0

    lax.fori_loop(0, slots, find_before, 0)
    lax.fori_loop(0, requests, find_last, 0)


def attention_constants(n, v):
    span, slots = v.pages.shape
    page_rows, _width, page_count = v.cache_v.shape
    requests = v.counts.shape[0]
    heads = n * n
    rows = v.place.shape[0]
    group = min(requests, heads)
    size = requests * group
    lane = lax.broadcasted_iota(jnp.int32, (rows, LANES), 1)
    v.place[...] = lane % span * page_rows + lane // span
    v.shift[...] = v.place[...] - lax.broadcasted_iota(jnp.int32, (rows, LANES), 0) // heads
    turn_row = lax.broadcasted_iota(jnp.int32, (size, size), 0)
    turn_col = lax.broadcasted_iota(jnp.int32, (size, size), 1)
    from_heads = jnp.where(turn_col == turn_row % group * requests + turn_row // group, 1.0, 0.0)
    v.turn[0] = from_heads.astype(bf16)
    to_heads = jnp.where(turn_row == turn_col % group * requests + turn_col // group, 1.0, 0.0)
    v.turn[1] = to_heads.astype(bf16)
    page_lane = lax.broadcasted_iota(jnp.int32, (span, page_count), 1)
    for s in range(0, slots, 2):
        pair = [jnp.where(v.pages[:, s + u : s + u + 1] == page_lane, 1.0, 0.0) for u in range(2)]
        v.sel[pl.ds(s * span, 2 * span), :] = jnp.concatenate(pair, axis=0).astype(bf16)
    v.acc[slots] = jnp.zeros(v.acc.shape[1:], f32)
    v.mrep[slots] = jnp.full(v.mrep.shape[1:], neg_floor, f32)
    v.lrep[slots] = jnp.zeros(v.lrep.shape[1:], f32)


def pick_rows(v, t):
    span, slots = v.pages.shape
    both = [
        lax.dot_general(v.sel[...], v.cache_v[2 * t + u], (((1,), (1,)), ((), ())), preferred_element_type=f32)
        for u in range(2)
    ]
    for s in range(slots):
        chunk = jnp.concatenate([one[s * span : (s + 1) * span] for one in both], axis=0)
        v.keys_v[s, pl.ds(pl.multiple_of(t * 2 * span, 2 * span), 2 * span), :] = chunk.astype(bf16)


def gather_part(n, v, x, y, c, first_peer, second_peer, partner, fetch):
    half = n // 2
    block_tiles = v.gathered.shape[2]
    g_ref, q_ref, other = v.gathered, v.q, v.other
    swap = send(q_ref, other, v.pair_send, v.pair_recv, partner)
    swap.start()
    attention_constants(n, v)
    swap.wait()

    def place(a, b):
        return ((x + a * (1 - c) + b * c + 2 * n) % n) * n + (y + a * c + b * (1 - c) + 2 * n) % n

    mine = place(0, 0)
    query_count, requests, held = q_ref.shape
    lane = lax.broadcasted_iota(jnp.int32, (requests, LANES), 1)
    tail = held % LANES
    pad = jnp.zeros((requests, LANES - tail), f32)
    tiles = []
    rotary = []
    for i in range(query_count):
        here = q_ref[i].astype(f32)
        there = other[i].astype(f32)
        low = jnp.concatenate([jnp.where(c == 0, here, there), pad], axis=1)
        high = jnp.concatenate([jnp.where(c == 0, there, here), pad], axis=1)
        full = held // LANES
        low = [low[:, t * LANES : (t + 1) * LANES] for t in range(full + 1)]
        high = [pltpu.roll(high[:, t * LANES : (t + 1) * LANES], tail, 1) for t in range(full + 1)]
        tiles += low[:full]
        left = low[full]
        for t in range(full):
            tiles.append(jnp.where(lane < tail, left, high[t]))
            left = high[t]
        rotary.append(jnp.where(lane < tail, left, jnp.where(lane < 2 * tail, high[full], 0.0)))
    tiles.append(rotary[0] + pltpu.roll(rotary[1], ROPE, 1))
    tiles.append(rotary[2])
    for t in range(block_tiles):
        g_ref[c, mine, t] = jnp.where(c == 0, tiles[t], tiles[block_tiles + t]).astype(bf16)

    def share(block):
        ref = g_ref.at[c, block]
        send(ref, ref, v.share_send, v.share_recv, partner).start()

    def to_right(block, index):
        ref = g_ref.at[c, block]
        send(ref, ref, v.right_send, v.right_recv.at[index], second_peer(1)).start()

    def to_left(block, index):
        ref = g_ref.at[c, block]
        send(ref, ref, v.left_send, v.left_recv.at[index], second_peer(-1)).start()

    own = g_ref.at[c, mine]
    for j in range(1, n):
        send(own, own, v.first_send, v.first_recv.at[j], first_peer(offset_of(j))).start()
    to_right(mine, 0)
    to_left(mine, 0)
    share(mine)

    def first_step(j, _):
        block = place(-offset_of(j), 0)
        ref = g_ref.at[c, block]
        send(ref, ref, v.first_send, v.first_recv.at[j], partner).wait_recv()
        to_right(block, j)
        to_left(block, j)
        share(block)
        return 0

    attention_tables(n, v)
    lax.fori_loop(1, n, first_step, 0)
    fetch.wait()
    pairs = v.cache_v.shape[0] // 2

    def take_right(s, j, forward):
        block = place(-offset_of(j), -s)
        ref = g_ref.at[c, block]
        send(ref, ref, v.right_send, v.right_recv.at[(s - 1) * n + j], partner).wait_recv()
        if forward:
            to_right(block, s * n + j)
        share(block)

    def take_left(s, j, forward):
        block = place(-offset_of(j), s)
        ref = g_ref.at[c, block]
        send(ref, ref, v.left_send, v.left_recv.at[(s - 1) * n + j], partner).wait_recv()
        if forward:
            to_left(block, s * n + j)
        share(block)

    for s in range(1, half + 1):
        if s == half:

            def last_step(j, _):
                take_right(half, j, False)
                take_left(half, j + half, False)
                return 0

            lax.fori_loop(0, half, last_step, 0)
        elif s == half - 1:

            def low_step(j, _):
                take_right(half - 1, j, True)
                take_left(half - 1, j, False)
                return 0

            def high_step(j, _):
                take_right(half - 1, j, False)
                take_left(half - 1, j, True)
                return 0

            lax.fori_loop(0, half, low_step, 0)
            lax.fori_loop(half, n, high_step, 0)
        else:

            def mid_step(j, _, s=s):
                take_right(s, j, True)
                take_left(s, j, True)
                if s == 1 and n == pairs:
                    pick_rows(v, j)
                return 0

            lax.fori_loop(0, n, mid_step, 0)

    if n != pairs or half < 3:
        for t in range(pairs):
            pick_rows(v, t)
    send(g_ref.at[1 - c], g_ref.at[1 - c], v.share_send, v.share_recv, partner).wait_recv()


def gather_sent(n, v, c, partner):
    half = n // 2
    ring_blocks = n * (half - 1) + half
    some = v.gathered.at[c, pl.ds(0, n - 1)]
    send(some, some, v.first_send, v.first_recv.at[0], partner).wait_send()
    some = v.gathered.at[c, pl.ds(0, ring_blocks)]
    send(some, some, v.right_send, v.first_recv.at[0], partner).wait_send()
    send(some, some, v.left_send, v.first_recv.at[0], partner).wait_send()
    send(v.gathered.at[c], v.gathered.at[c], v.share_send, v.share_recv, partner).wait_send()


def attend_part(n, latent, v, c):
    heads = n * n
    block_tiles, requests = v.gathered.shape[2], v.gathered.shape[3]
    span, slots = v.pages.shape
    page_rows, width, page_count = v.cache_v.shape
    latent_tiles = latent // LANES
    query_count = v.q.shape[0]
    group = min(requests, heads)
    unroll = min(slots, 4)

    def spread(block, _):
        h = block * group
        for i in range(query_count):
            base = pl.multiple_of(i * heads + h, group)

            def turned(t):
                stack = jnp.concatenate(
                    [v.gathered[t // block_tiles, h + u, t % block_tiles] for u in range(group)], axis=0
                )
                return jnp.dot(v.turn[0], stack, preferred_element_type=f32)

            def keep(t, tile):
                for r in range(requests):
                    v.qr[r, pl.ds(base, group), pl.ds(t * LANES, LANES)] = tile[r * group : (r + 1) * group].astype(bf16)

            for t in range(latent_tiles):
                keep(t, turned(i * latent_tiles + t))
            rotary = turned(query_count * latent_tiles + i // 2)
            keep(latent_tiles, pltpu.roll(rotary, ROPE, 1) if i % 2 else rotary)
        return 0

    lax.fori_loop(0, heads // group, spread, 0)

    def slot_step(g, _):
        held = []
        for u in range(unroll):
            s = g * unroll + u
            r = v.req[s]
            scores = (
                lax.dot_general(
                    v.qr[r, :, :width], v.keys_v[s], (((1,), (1,)), ((), ())), preferred_element_type=f32
                )
                * softmax_scale
            )
            limit = (v.counts[r] - v.start[s]) * page_rows - (query_count - 1)
            visible = (v.place[...] < v.live[s] * page_rows) & (v.shift[...] < limit)
            slot_max = jnp.max(jnp.where(visible, scores, neg_floor), axis=1, keepdims=True)
            weights = jnp.exp(jnp.where(visible, scores - slot_max, neg_floor))
            slot_sum = jnp.sum(weights, axis=1, keepdims=True)
            held.append((weights.astype(bf16), slot_max, slot_sum))
        for u in range(unroll):
            s = g * unroll + u
            p = v.before[s]
            weights, slot_max, slot_sum = held[u]
            old = v.mrep[p]
            new = jnp.maximum(old, slot_max)
            kept = jnp.exp(old - new)
            added = jnp.exp(slot_max - new)
            v.mrep[s] = new
            v.lrep[s] = v.lrep[p] * kept + added * slot_sum
            for t in range(0, latent_tiles, 2):
                out = jnp.dot(weights, v.keys_v[s, :, t * LANES : (t + 2) * LANES], preferred_element_type=f32)
                for w in range(2):
                    v.acc[s, t + w] = v.acc[p, t + w] * kept + out[:, w * LANES : (w + 1) * LANES] * added
        return 0

    lax.fori_loop(0, slots // unroll, slot_step, 0)
    last = [v.last[r] for r in range(requests)]
    head_lane = lax.broadcasted_iota(jnp.int32, (heads, LANES), 1)
    stats = jnp.zeros((heads, LANES), f32)
    for i in range(query_count):
        for r in range(requests):
            at = pl.ds(i * heads, heads)
            stats = jnp.where(head_lane == i * requests + r, v.mrep[last[r], at, :], stats)
            stats = jnp.where(head_lane == (query_count + i) * requests + r, v.lrep[last[r], at, :], stats)
    v.flat[...] = stats
    for a in range(n):
        v.stat[0, a] = v.flat[pl.ds(a * n, n), :]
        v.stat[1, a] = v.flat[pl.ds(a, n, stride=n), :]


def put_side(n, latent, v, side):
    heads = n * n
    requests = v.counts.shape[0]
    query_count = v.q.shape[0]
    group = min(requests, heads)
    side_tiles = latent // LANES // 2
    last = [v.last[r] for r in range(requests)]

    def put(block, _):
        h = block * group
        for i in range(query_count):
            base = pl.multiple_of(i * heads + h, group)
            for t in range(side_tiles):
                tile = side * side_tiles + t
                stack = jnp.concatenate(
                    [v.acc[last[r], tile, pl.ds(base, group), :] for r in range(requests)], axis=0
                )
                flat = jnp.dot(v.turn[1], stack.astype(bf16), preferred_element_type=f32).astype(bf16)
                for u in range(group):
                    high, low = (h + u) // n, (h + u) % n
                    a = high * (1 - side) + low * side
                    b = low * (1 - side) + high * side
                    v.part[side, a, b, i, :, pl.ds(t * LANES, LANES)] = flat[u * requests : (u + 1) * requests]
        return 0

    lax.fori_loop(0, heads // group, put, 0)


def combine_part(n, v, x, y, c, first_peer, second_peer, partner):
    a_here = x * (1 - c) + y * c
    b_here = y * (1 - c) + x * c
    _h, query_count, requests, cols = v.chip_part.shape[1:]
    m_lanes = query_count * requests
    order = list(range(n - 1, -1, -1))

    def a_at(d):
        return (a_here + d + n) % n

    def b_at(d):
        return (b_here + d + n) % n

    stat_swap = send(v.stat.at[1 - c], v.pair_stat, v.sem_pair_stat.at[0], v.sem_pair_stat.at[1], partner)
    stat_swap.start()
    put_side(n, 2 * cols, v, 1 - c)
    for j in order:
        a_pair = (b_here + offset_of(j) + n) % n
        send(
            v.part.at[1 - c, a_pair], v.pair_part.at[a_pair], v.sem_pair_part.at[0, j], v.sem_pair_part.at[1, j], partner
        ).start()
    put_side(n, 2 * cols, v, c)
    stat_swap.wait()

    lane8 = lax.broadcasted_iota(jnp.int32, (n, LANES), 1)
    lane16 = lax.broadcasted_iota(jnp.int32, (requests, LANES), 1)
    row16 = lax.broadcasted_iota(jnp.int32, (requests, LANES), 0)

    def column(row, base):
        picked = jnp.where(lane16 == row16 + base, jnp.broadcast_to(row, (requests, LANES)), 0.0)
        return jnp.sum(picked, axis=1, keepdims=True)

    def merged(all_stats):
        best = all_stats[0]
        for one in all_stats[1:]:
            best = jnp.maximum(best, one)
        factors = [jnp.exp(one - best) for one in all_stats]
        denom = 0.0
        for factor, one in zip(factors, all_stats):
            denom = denom + pltpu.roll(factor, m_lanes, 1) * one
        return factors, jnp.where(lane8 < m_lanes, best, denom)

    for a in range(n):
        factors, stats = merged([v.stat[c, a], v.pair_stat[a]])
        v.f_mine[a] = factors[0]
        v.f_pair[a] = factors[1]
        v.chip_stat[a] = stats
    for j in order[:-1]:
        send(
            v.chip_stat.at[a_at(offset_of(j))], v.ring_stat.at[j], v.sem_stat_a.at[0, j], v.sem_stat_a.at[1, j],
            first_peer(offset_of(j)),
        ).start()
    v.ring_stat[0] = v.chip_stat[a_here]
    half = n // 2
    signs = (1, -1)
    row8 = lax.broadcasted_iota(jnp.int32, (n, LANES), 0)
    far = row8 < 0
    for j in range(half, n):
        far = far | (row8 == b_at(offset_of(j)))

    def pair_chunk(j):
        a_pair = (b_here + offset_of(j) + n) % n
        a = a_at(offset_of(j))
        send(
            v.part.at[1 - c, a_pair], v.pair_part.at[a], v.sem_pair_part.at[0, j], v.sem_pair_part.at[1, j], partner
        ).wait()
        f_m = v.f_mine[a]
        f_p = v.f_pair[a]
        for b in range(n):
            for i in range(query_count):
                mine = v.part[c, a, b, i].astype(f32) * column(f_m[b : b + 1], i * requests)
                theirs = v.pair_part[a, b, i].astype(f32) * column(f_p[b : b + 1], i * requests)
                v.chip_part[a, b, i] = (mine + theirs).astype(bf16)

    def chain_block(side, step, j, src):
        return send(
            src, v.chain_in.at[side, step - 1, b_at(offset_of(j))], v.sem_chain.at[0, side, step - 1, j],
            v.sem_chain.at[1, side, step - 1, j], first_peer(signs[side]),
        )

    def chain_best(side, step):
        return send(
            v.best_out.at[side, step - 1], v.best_in.at[side, step - 1], v.sem_best.at[0, side, step - 1],
            v.sem_best.at[1, side, step - 1], first_peer(signs[side]),
        )

    def chain_first():
        a = a_at(half)
        for side in range(2):
            mine = far if side == 0 else ~far
            v.best_out[side, 0] = jnp.where(mine, v.chip_stat[a], neg_floor)
            chain_best(side, 1).start()

        def both(k, _):
            for side in range(2):
                j = (n - 1 if side == 0 else half - 1) - k
                chain_block(side, 1, j, v.chip_part.at[a, b_at(offset_of(j))]).start()
            return 0

        lax.fori_loop(0, half, both, 0)

    def chain_join(side, step, j, a):
        chain_block(side, step - 1, j, v.chip_part.at[0, 0]).wait_recv()
        b = b_at(offset_of(j))
        f_in = v.f_chain[side, 0, pl.ds(b, 1), :]
        f_own = v.f_chain[side, 1, pl.ds(b, 1), :]
        for i in range(query_count):
            came = v.chain_in[side, step - 2, b, i].astype(f32) * column(f_in, i * requests)
            mine = v.chip_part[a, b, i].astype(f32) * column(f_own, i * requests)
            v.chain_out[side, step - 2, b, i] = (came + mine).astype(bf16)
        chain_block(side, step, j, v.chain_out.at[side, step - 2, b]).start()

    def chain_step(step):
        targets = [a_at(signs[side] * (half + 1 - step)) for side in range(2)]
        if step == 2:

            def alone(k, _):
                for side in range(2):
                    j = (half - 1 if side == 0 else n - 1) - k
                    chain_block(side, 2, j, v.chip_part.at[targets[side], b_at(offset_of(j))]).start()
                return 0

            lax.fori_loop(0, half, alone, 0)
        for side in range(2):
            chain_best(side, step - 1).wait_recv()
            came = v.best_in[side, step - 2]
            mine = v.chip_stat[targets[side]]
            best = jnp.maximum(came, mine)
            v.f_chain[side, 0] = jnp.exp(came - best)
            v.f_chain[side, 1] = jnp.exp(mine - best)
            v.best_out[side, step - 1] = best
            chain_best(side, step).start()
        if step == 2:

            def joined(k, _):
                for side in range(2):
                    chain_join(side, 2, (n - 1 if side == 0 else half - 1) - k, targets[side])
                return 0

            lax.fori_loop(0, half, joined, 0)
        else:

            def joined(k, _):
                for side in range(2):
                    chain_join(side, step, n - 1 - k, targets[side])
                return 0

            lax.fori_loop(0, n, joined, 0)

    def ring_stats():
        for j in range(1, n):
            send(
                v.chip_stat.at[a_here], v.ring_stat.at[j], v.sem_stat_a.at[0, j], v.sem_stat_a.at[1, j],
                first_peer(offset_of(j)),
            ).wait()
        _factors, stats = merged([v.ring_stat[j] for j in range(n)])
        v.col_stat_send[...] = stats
        for j in order[:-1]:
            send(
                v.col_stat_send, v.col_stat.at[j], v.sem_stat_b.at[0, j], v.sem_stat_b.at[1, j],
                second_peer(offset_of(j)),
            ).start()
        v.col_stat[0] = stats

    def column_stats():
        for j in range(1, n):
            send(
                v.col_stat_send, v.col_stat.at[j], v.sem_stat_b.at[0, j], v.sem_stat_b.at[1, j],
                second_peer(offset_of(j)),
            ).wait()
        factors, stats = merged([v.col_stat[j] for j in range(n)])
        for j in range(n):
            v.f_col[j] = factors[j]
        v.f_col[n] = stats
        lse = stats + jnp.log(pltpu.roll(jnp.where(lane8 < m_lanes, 1.0, stats), LANES - m_lanes, 1))
        v.lse_send[...] = lse
        v.lse_all[a_here] = lse
        for j in range(1, n):
            send(
                v.lse_send, v.lse_all.at[a_here], v.sem_lse.at[0, j], v.sem_lse.at[1, j], first_peer(offset_of(j))
            ).start()

    pair_chunk(n - 1)
    chain_first()
    for step in range(2, half + 1):
        pair_chunk(2 * (half + 1 - step))
        pair_chunk(2 * (half + 1 - step) - 1)
        chain_step(step)
        if step == 2:
            ring_stats()
    column_stats()
    pair_chunk(0)
    for side in range(2):
        chain_best(side, half).wait_recv()
    best = v.col_stat_send[...]
    v.f_ring[0] = jnp.exp(v.chip_stat[a_here] - best)
    for side in range(2):
        v.f_ring[1 + side] = jnp.exp(v.best_in[side, half - 1] - best)

    def finish(j):
        b = b_at(offset_of(j))
        rows = [v.f_ring[k, pl.ds(b, 1), :] for k in range(3)]
        for side in range(2):
            chain_block(side, half, j, v.chip_part.at[0, 0]).wait_recv()
        for i in range(query_count):
            total = v.chip_part[a_here, b, i].astype(f32) * column(rows[0], i * requests)
            for side in range(2):
                came = v.chain_in[side, half - 1, b, i].astype(f32)
                total = total + came * column(rows[1 + side], i * requests)
            v.col_send_part[b, i] = total.astype(bf16)

    def finish_far(k, _):
        j = n - 1 - k
        finish(j)
        send(
            v.col_send_part.at[b_at(offset_of(j))], v.col_part.at[j], v.sem_part_b.at[0, j], v.sem_part_b.at[1, j],
            second_peer(offset_of(j)),
        ).start()
        return 0

    lax.fori_loop(0, n - 1, finish_far, 0)
    finish(0)
    sums = [0.0] * query_count
    for j in range(n):
        if j:
            send(
                v.col_send_part.at[b_here], v.col_part.at[j], v.sem_part_b.at[0, j], v.sem_part_b.at[1, j],
                second_peer(offset_of(j)),
            ).wait()
        row = v.f_col[j, pl.ds(b_here, 1), :]
        for i in range(query_count):
            block = v.col_send_part[b_here, i] if j == 0 else v.col_part[j, i]
            sums[i] = sums[i] + block.astype(f32) * column(row, i * requests)
    row = v.f_col[n, pl.ds(b_here, 1), :]
    for i in range(query_count):
        v.out[i] = (sums[i] / column(row, m_lanes + i * requests)).astype(bf16)
    for side in range(2):
        for step in range(1, half + 1):
            chain_best(side, step).wait_send()

            def sent(j, _, side=side, step=step):
                chain_block(side, step, j, v.chip_part.at[0, 0]).wait_send()
                return 0

            first = half if (step, side) == (1, 0) else 0
            end = half if (step, side) == (1, 1) else n
            lax.fori_loop(first, end, sent, 0)
    for j in range(1, n):
        a_from = a_at(-offset_of(j))
        send(
            v.lse_send, v.lse_all.at[a_from], v.sem_lse.at[0, j], v.sem_lse.at[1, j], first_peer(offset_of(j))
        ).wait()
    heads = n * n
    for a in range(n):
        v.flat[pl.ds(a * n, n), :] = v.lse_all[a]
    turned = jnp.concatenate([v.flat[pl.ds(a, n, stride=n), :] for a in range(n)], axis=0)
    lse = jnp.where(c == 0, v.flat[...], turned)
    if heads < LANES:
        lse = jnp.concatenate([lse, jnp.zeros((LANES - heads, LANES), f32)], axis=0)
    lse = jnp.transpose(lse)
    for i in range(query_count):
        v.lse[i] = lse[i * requests : (i + 1) * requests, :heads]


def decode(q, cache, pages, tables, n, latent):
    query_count, requests, _held = q.shape
    page_rows, width, page_count = cache.shape
    span, slots = pages.shape
    heads = n * n
    rows = heads * query_count
    cols = latent // 2
    tiles = latent // LANES
    block_tiles = (query_count * tiles + 2) // 2
    size = requests * min(requests, heads)
    dma = pltpu.SemaphoreType.DMA
    vmem = pl.BlockSpec(memory_space=pltpu.VMEM)
    smem = pl.BlockSpec(memory_space=pltpu.SMEM)
    block = (n, n, query_count, requests, cols)
    one = (n, query_count, requests, cols)
    scratch = dict(
        cache_v=pltpu.VMEM(cache.shape, bf16),
        cache_sem=dma,
        gathered=pltpu.VMEM((2, heads, block_tiles, requests, LANES), bf16),
        other=pltpu.VMEM(q.shape, bf16),
        before=pltpu.SMEM((slots,), jnp.int32),
        last=pltpu.SMEM((requests,), jnp.int32),
        pair_send=dma, pair_recv=dma, first_send=dma, first_recv=dma((n,)), right_send=dma,
        right_recv=dma((n * n // 2,)), left_send=dma, left_recv=dma((n * n // 2,)), share_send=dma, share_recv=dma,
        sel=pltpu.VMEM((slots * span, page_count), bf16),
        keys_v=pltpu.VMEM((slots, page_rows * span, width), bf16),
        qr=pltpu.VMEM((requests, rows, (tiles + 1) * LANES), bf16),
        acc=pltpu.VMEM((slots + 1, tiles, rows, LANES), f32),
        mrep=pltpu.VMEM((slots + 1, rows, LANES), f32),
        lrep=pltpu.VMEM((slots + 1, rows, LANES), f32),
        turn=pltpu.VMEM((2, size, size), bf16),
        place=pltpu.VMEM((rows, LANES), jnp.int32),
        shift=pltpu.VMEM((rows, LANES), jnp.int32),
        flat=pltpu.VMEM((heads, LANES), f32),
        part=pltpu.VMEM((2,) + block, bf16),
        stat=pltpu.VMEM((2, n, n, LANES), f32),
        pair_part=pltpu.VMEM(block, bf16),
        pair_stat=pltpu.VMEM((n, n, LANES), f32),
        f_mine=pltpu.VMEM((n, n, LANES), f32),
        f_pair=pltpu.VMEM((n, n, LANES), f32),
        chip_part=pltpu.VMEM(block, bf16),
        chip_stat=pltpu.VMEM((n, n, LANES), f32),
        chain_in=pltpu.VMEM((2, n // 2) + one, bf16),
        chain_out=pltpu.VMEM((2, n // 2) + one, bf16),
        best_in=pltpu.VMEM((2, n // 2, n, LANES), f32),
        best_out=pltpu.VMEM((2, n // 2, n, LANES), f32),
        f_chain=pltpu.VMEM((2, 2, n, LANES), f32),
        ring_stat=pltpu.VMEM((n, n, LANES), f32),
        f_ring=pltpu.VMEM((3, n, LANES), f32),
        col_send_part=pltpu.VMEM(one, bf16),
        col_stat_send=pltpu.VMEM((n, LANES), f32),
        col_part=pltpu.VMEM(one, bf16),
        col_stat=pltpu.VMEM((n, n, LANES), f32),
        f_col=pltpu.VMEM((n + 1, n, LANES), f32),
        lse_send=pltpu.VMEM((n, LANES), f32),
        lse_all=pltpu.VMEM((n, n, LANES), f32),
        sem_pair_stat=dma((2,)),
        sem_pair_part=dma((2, n)), sem_stat_a=dma((2, n)), sem_chain=dma((2, 2, n // 2, n)), sem_best=dma((2, 2, n // 2)), sem_stat_b=dma((2, n)),
        sem_part_b=dma((2, n)), sem_lse=dma((2, n)),
    )
    names = ["q", "cache", "pages", "req", "start", "live", "counts", "out", "lse"] + list(scratch)
    return pl.pallas_call(
        functools.partial(decode_kernel, n, latent, names),
        out_shape=(
            jax.ShapeDtypeStruct((query_count, requests, cols), bf16),
            jax.ShapeDtypeStruct((query_count, requests, heads), f32),
        ),
        in_specs=[vmem, pl.BlockSpec(memory_space=pl.ANY), vmem] + [smem] * 4,
        out_specs=(vmem, vmem),
        scratch_shapes=list(scratch.values()),
        compiler_params=pltpu.CompilerParams(
            collective_id=0, has_side_effects=True, vmem_limit_bytes=62 * 2**20
        ),
        name="decode",
    )(q, cache, pages, *tables)


def per_device(n, queries, cache, page_counts, slot_request, slot_start, slot_live, slot_pages):
    latent = cache.shape[2] - ROPE
    tables = (slot_request, slot_start, slot_live, page_counts)
    out, lse = decode(
        jnp.transpose(queries, (1, 0, 2)), jnp.transpose(cache, (1, 2, 0)), slot_pages.T, tables, n, latent
    )
    return jnp.transpose(out, (1, 0, 2)), jnp.transpose(lse, (1, 0, 2))


def solution(mesh):
    n = round((mesh.shape["kv"] // 2) ** 0.5)
    split = Mesh(mesh.devices.reshape(mesh.shape["rep"], n, n, 2), REP_KV)
    placed = (
        P("rep", None, KV),
        P(REP_KV, None, None),
        P("rep"),
        P(REP_KV),
        P(REP_KV),
        P(REP_KV),
        P(REP_KV, None),
    )
    return jax.shard_map(
        functools.partial(per_device, n),
        mesh=split,
        in_specs=placed,
        out_specs=(P("rep", None, KV), P("rep", None, None)),
        check_vma=False,
    )
```
